256 devices in a mesh: row: 8 (over y, z_lo), col: 32 (over x, z_hi, core).
Axes of the slice: x: 4, y: 4, z: 8 (z_hi: 4, z_lo: 2; z = z_hi * 2 + z_lo), core: 2. Of those that a mesh axis runs over, the one named last changes fastest.
Arguments:
- x_field: bfloat16 [131072, 256], P('col'), may hold values from -6 to 6
- observed: bfloat16 [8192, 256], P(('row', 'col')), may hold values from -6 to 6
- sat_scale: float32 [256], replicated, may hold values from 0.5 to 4
- u_coef: bfloat16 [16, 256, 512, 256], P('row', 'col'), may hold values from -0.03125 to 0.03125
- v_coef: bfloat16 [16, 256, 512, 256], P('row', 'col'), may hold values from -0.25 to 0.25
- ranks: int32 [16, 256], P('row', 'col'), may hold values from 16 to 256
Outputs:
- gradient: bfloat16 [131072, 256], P('col')
The draws below stay inside these ranges and needn't reach their ends.
All inputs are finite; a program needn't handle non-finite values.
Results may differ from the reference program's by a relative error of at most 0.0065.
Values may be sent and summed in bfloat16 or wider, within the bound.
A program may use at most 64 MiB of HBM per device.

```python
import math
import jax
import jax.numpy as jnp
from jax import lax

TILE = 512
RMAX = 256
S = 256
NT_ROWS = 16
NT_COLS = 256
ROWS = 8192
NCOLS = 131072


def plant(values, own_key, low, largest):
    spot = [jax.random.randint(jax.random.fold_in(own_key, axis), (), 0, length) for axis, length in enumerate(values.shape)]
    widest = values.shape.index(max(values.shape))
    beside = spot[:widest] + [(spot[widest] + 1) % values.shape[widest]] + spot[widest + 1:]
    return values.at[tuple(spot)].set(low).at[tuple(beside)].set(largest)


def block_scale(rng, extent, pieces, least, top_value):
    loudness, own = 1.0, jax.random.fold_in(rng, 6)
    for dim, parts in pieces:
        draws = jnp.exp(jax.random.uniform(jax.random.fold_in(own, dim), (parts,), jnp.float32, least / len(pieces), top_value / len(pieces)))
        loudness = loudness * jnp.repeat(draws, extent[dim] // parts).reshape([-1 if axis == dim else 1 for axis in range(len(extent))])
    return loudness


def centred(rng, dims, deviation, limit, pieces=(), held_as=jnp.bfloat16):
    array = jax.random.normal(rng, dims, jnp.float32) * deviation
    if len(pieces) > 0:
        array = block_scale(rng, dims, pieces, -0.22, 0.18) * array
    return jnp.clip(array, min=-limit, max=limit).astype(held_as)


def setup_inputs(seed: int = 0) -> dict:
    key_list = jax.random.split(jax.random.key(seed), 7)
    x_field = centred(key_list[0], (NCOLS, S), 1.0, 6.0, ((0, 32),))
    observed = centred(key_list[1], (ROWS, S), 1.0, 6.0, ((0, 256),))
    sat_scale = jnp.clip(jnp.exp(jax.random.uniform(key_list[2], (S,), jnp.float32, math.log(0.5), math.log(4.0))), 0.5, 4.0)
    u_coef = centred(key_list[3], (NT_ROWS, NT_COLS, TILE, RMAX), (NT_COLS * RMAX // 2) ** -0.5, 0.03125, ((0, 8), (1, 32)))
    v_coef = centred(key_list[4], (NT_ROWS, NT_COLS, TILE, RMAX), TILE ** -0.5, 0.25, ((0, 8), (1, 32)))
    ranks = plant(jax.random.randint(key_list[5], (NT_ROWS, NT_COLS), RMAX // 16, RMAX + 1), jax.random.fold_in(key_list[5], 1), RMAX // 16, RMAX).astype(jnp.int32)
    return {"x_field": x_field, "observed": observed, "sat_scale": sat_scale, "u_coef": u_coef, "v_coef": v_coef, "ranks": ranks}


def reference(x_field, observed, sat_scale, u_coef, v_coef, ranks):
    source_tiles = x_field.astype(jnp.float32).reshape(NT_COLS, TILE, S)
    rank_mask = (jnp.arange(RMAX, dtype=jnp.int32)[None, None, :] < ranks[:, :, None]).astype(jnp.float32)[..., None]

    def forward_row(packed):
        u_tile, v_tile, mask_row = packed
        coeffs = jnp.einsum("jtk,jts->jks", v_tile.astype(jnp.float32), source_tiles)
        coeffs = (coeffs * mask_row).astype(jnp.bfloat16)
        return jnp.einsum("jtk,jks->ts", u_tile.astype(jnp.float32), coeffs.astype(jnp.float32))

    predicted = lax.map(forward_row, (u_coef, v_coef, rank_mask)).reshape(ROWS, S)
    misfit = (predicted - observed.astype(jnp.float32)) / sat_scale
    residual = (sat_scale * jnp.tanh(misfit)).astype(jnp.bfloat16)
    resid_tiles = residual.reshape(NT_ROWS, TILE, S)

    def adjoint_row(running, packed):
        u_tile, v_tile, mask_row, resid_row = packed
        adjoint = jnp.einsum("jtk,ts->jks", u_tile.astype(jnp.float32), resid_row.astype(jnp.float32))
        adjoint = (adjoint * mask_row).astype(jnp.bfloat16)
        return running + jnp.einsum("jtk,jks->jts", v_tile.astype(jnp.float32), adjoint.astype(jnp.float32)), None

    gradient, _ = lax.scan(adjoint_row, jnp.zeros((NT_COLS, TILE, S), jnp.float32), (u_coef, v_coef, rank_mask, resid_tiles))
    return gradient.reshape(NCOLS, S).astype(jnp.bfloat16)
```

```python
import functools

import jax
import jax.numpy as jnp
from jax import lax
from jax.experimental import pallas as pl
from jax.experimental.pallas import tpu as pltpu
from jax.sharding import PartitionSpec as P

MESH = pl.DeviceIdType.MESH
F32, BF16 = jnp.float32, jnp.bfloat16

CHUNKS = (
    (0, 512, (0, 1, 2)),
    (512, 512, (1, 2, 0)),
    (1024, 512, (2, 0, 1)),
    (1536, 512, (0, 1, 2)),
    (2048, 512, (1, 2, 0)),
    (2560, 512, (2, 0, 1)),
    (3072, 384, (0, 1, 2)),
    (3712, 384, (1, 2, 0)),
    (3456, 256, (2, 0, 1)),
)
READY = {0: (0,), 1: (1,), 2: (2,), 3: (3,), 4: (4,), 5: (5,), 6: (6,), 7: (7, 8)}
OFFSETS = tuple((dx, dz) for dx in (2, 1, 3, 0) for dz in (2, 1, 3, 0) if (dx, dz) != (0, 0))


def matmul(a, b):
    return lax.dot_general(a, b, (((1,), (0,)), ((), ())), preferred_element_type=F32)


def matmul_t(a, b):
    return lax.dot_general(a, b, (((1,), (1,)), ((), ())), preferred_element_type=F32)


def event_order(n):
    events = []
    for i in range(n):
        wave = i // 3
        for stage in range(6):
            events.append((stage * 3 + wave * 3 + (2 if stage > 2 else 0), stage, i))
    return [(stage, i) for _, stage, i in sorted(events)]


def kernel(
    x_hbm, obs_hbm, sat_hbm, u_hbm, v_hbm, ranks_hbm, out,
    xb, ub, vb, obs, sat, ranks, xt, part, recv_core, send_a, recv_a, resid, resid_t, grad,
    send1, send2, send3, recv1, recv2, recv3,
    load_sem, small_sem, core_send, core_recv, a_send, a_recv, b_send, b_recv, row_send, row_recv,
):
    r, c = lax.axis_index("row"), lax.axis_index("col")
    y, zl = r // 2, r % 2
    x, zh, k = c // 8, (c % 8) // 2, c % 2
    here = x * 4 + zh
    tile_rows, tile_cols = ub.shape[0], ub.shape[1]

    row_peer = (
        (y * 2 + 1 - zl, c),
        ((y + 1 - 2 * (y % 2)) * 2 + zl, c),
        ((3 - y) * 2 + zl, c),
    )
    bits = (zl, ((y + 1) // 2) % 2, y // 2)
    core_peer = (r, c + 1 - 2 * k)

    def chip_at(dx, dz):
        return ((x + dx) % 4) * 4 + (zh + dz) % 4

    barrier = pltpu.get_barrier_semaphore()
    peers = [core_peer, *row_peer] + [(r, chip_at(dx, dz) * 2 + k) for dx, dz in OFFSETS]
    for peer in peers:
        pl.semaphore_signal(barrier, inc=1, device_id=peer, device_id_type=MESH)

    def v_load(a, j):
        return pltpu.make_async_copy(v_hbm.at[a, j], vb.at[a, j], load_sem.at[0, a * tile_cols + j])

    def u_load(a, j):
        return pltpu.make_async_copy(u_hbm.at[a, j], ub.at[a, j], load_sem.at[1, a * tile_cols + j])

    def x_load(j):
        return pltpu.make_async_copy(x_hbm.at[pl.ds(j * 512, 512)], xb.at[j], load_sem.at[2, j])

    small = (
        pltpu.make_async_copy(ranks_hbm, ranks, small_sem.at[0]),
        pltpu.make_async_copy(obs_hbm, obs, small_sem.at[1]),
        pltpu.make_async_copy(sat_hbm, sat, small_sem.at[2]),
    )
    small[0].start()
    for j in range(tile_cols):
        x_load(j).start()
        v_load(0, j).start()
        u_load(0, j).start()
    for j in range(tile_cols):
        v_load(1, j).start()
        u_load(1, j).start()
    small[1].start()
    small[2].start()

    eye = (
        lax.broadcasted_iota(jnp.int32, (256, 256), 0) == lax.broadcasted_iota(jnp.int32, (256, 256), 1)
    ).astype(F32).astype(BF16)
    lane = lax.broadcasted_iota(jnp.int32, (256, 256), 1)

    def masked(value, a, j):
        return jnp.where(lane < ranks[a, j], value, 0.0).astype(BF16)

    small[0].wait()
    core_copies = []
    for a in range(tile_rows):
        for j in range(tile_cols):
            if a == 0:
                x_load(j).wait()
                xt[j] = matmul_t(eye, xb[j]).astype(BF16)
            v_load(a, j).wait()
            coeffs = masked(matmul(xt[j], vb[a, j]), a, j)
            u_load(a, j).wait()
            term = matmul_t(ub[a, j], coeffs).reshape(8, 2, 32, 256)
            if j == 0:
                part[pl.ds(a * 8, 8)] = term
            else:
                part[pl.ds(a * 8, 8)] += term
        if a == 0:
            pl.semaphore_wait(barrier, len(peers))
        copy = pltpu.make_async_remote_copy(
            src_ref=part.at[pl.ds(a * 8, 8), 1 - k],
            dst_ref=recv_core.at[pl.ds(a * 8, 8)],
            send_sem=core_send.at[a],
            recv_sem=core_recv.at[a],
            device_id=core_peer,
            device_id_type=MESH,
        )
        copy.start()
        core_copies.append(copy)

    for a in range(tile_rows):
        core_copies[a].wait_recv()
        blocks = pl.ds(a * 8, 8)
        send_a[blocks] = (part[blocks, k] + recv_core[blocks]).astype(BF16)

    a_copies = []
    for n, (dx, dz) in enumerate(OFFSETS):
        there = chip_at(dx, dz)
        copy = pltpu.make_async_remote_copy(
            src_ref=send_a.at[there],
            dst_ref=recv_a.at[n],
            send_sem=a_send.at[n],
            recv_sem=a_recv.at[n],
            device_id=(r, there * 2 + k),
            device_id_type=MESH,
        )
        copy.start()
        a_copies.append(copy)

    small[1].wait()
    small[2].wait()
    predicted = part[here, k] + recv_core[here]
    for n, copy in enumerate(a_copies):
        copy.wait_recv()
        predicted = predicted + recv_a[n].astype(F32)
    scale = sat[...].reshape(1, 256)
    misfit = (predicted - obs[...].astype(F32)) / scale
    resid[here, k] = (scale * jnp.tanh(misfit)).astype(BF16)

    b_copies = []
    for n, (dx, dz) in enumerate(OFFSETS):
        copy = pltpu.make_async_remote_copy(
            src_ref=resid.at[here, k],
            dst_ref=resid.at[here, k],
            send_sem=b_send.at[n],
            recv_sem=b_recv.at[n],
            device_id=(r, chip_at(dx, dz) * 2 + k),
            device_id_type=MESH,
        )
        copy.start()
        b_copies.append(copy)
    for copy in core_copies + a_copies:
        copy.wait_send()
    for copy in b_copies:
        copy.wait_recv()
    copy = pltpu.make_async_remote_copy(
        src_ref=resid.at[:, k],
        dst_ref=resid.at[:, k],
        send_sem=core_send.at[2],
        recv_sem=core_recv.at[2],
        device_id=core_peer,
        device_id_type=MESH,
    )
    copy.start()
    for other in b_copies:
        other.wait_send()
    copy.wait()

    for a in range(tile_rows):
        resid_t[a] = matmul_t(eye, resid[pl.ds(a * 8, 8)].reshape(512, 256)).astype(BF16)

    sends = [(send1, recv1), (send2, recv2), (send3, recv3)]

    def base_of(i, depth):
        first, rows, dims = CHUNKS[i]
        base = first
        for d in range(depth):
            base = base + bits[dims[d]] * (rows >> (d + 1))
        return base if depth == 0 else pl.multiple_of(base, 16)

    def reduce_copy(i, step):
        first, rows, dims = CHUNKS[i]
        slot = pl.ds(first >> (step + 1), rows >> (step + 1))
        return pltpu.make_async_remote_copy(
            src_ref=sends[step][0].at[slot],
            dst_ref=sends[step][1].at[slot],
            send_sem=row_send.at[i, step],
            recv_sem=row_recv.at[i, step],
            device_id=row_peer[dims[step]],
            device_id_type=MESH,
        )

    def gather_copy(i, step):
        first, rows, dims = CHUNKS[i]
        where = pl.ds(base_of(i, step + 1), rows >> (step + 1))
        return pltpu.make_async_remote_copy(
            src_ref=out.at[where],
            dst_ref=out.at[where],
            send_sem=row_send.at[i, 3 + step],
            recv_sem=row_recv.at[i, 3 + step],
            device_id=row_peer[dims[step]],
            device_id_type=MESH,
        )

    def send_part(i, step):
        first, rows, dims = CHUNKS[i]
        half = rows >> (step + 1)
        bit = bits[dims[step]]
        theirs = pl.multiple_of((1 - bit) * half, 16)
        base = base_of(i, step)
        value = grad[pl.ds(pl.multiple_of(base + theirs, 16), half)]
        slot = first >> (step + 1)
        if step > 0:
            value = value + sends[step - 1][1][pl.ds(pl.multiple_of((first >> step) + theirs, 16), half)].astype(F32)
        sends[step][0][pl.ds(slot, half)] = value.astype(BF16)
        reduce_copy(i, step).start()
        if step > 0:
            mine = pl.multiple_of(bit * half, 16)
            keep = pl.ds(pl.multiple_of(base + mine, 16), half)
            grad[keep] = grad[keep] + sends[step - 1][1][
                pl.ds(pl.multiple_of((first >> step) + mine, 16), half)
            ].astype(F32)

    for j in range(tile_cols):
        total = None
        for a in range(tile_rows):
            adjoint = masked(matmul(resid_t[a], ub[a, j]), a, j)
            term = matmul_t(vb[a, j], adjoint)
            total = term if total is None else total + term
        grad[pl.ds(j * 512, 512)] = total
        for i in READY[j]:
            send_part(i, 0)

    for stage, i in event_order(len(CHUNKS)):
        first, rows, dims = CHUNKS[i]
        if stage < 2:
            reduce_copy(i, stage).wait_recv()
            send_part(i, stage + 1)
        elif stage == 2:
            reduce_copy(i, 2).wait_recv()
            where = pl.ds(base_of(i, 3), rows >> 3)
            out[where] = (grad[where] + recv3[pl.ds(first >> 3, rows >> 3)].astype(F32)).astype(BF16)
            gather_copy(i, 2).start()
        else:
            step = 5 - stage
            gather_copy(i, step).wait_recv()
            if step > 0:
                gather_copy(i, step - 1).start()
    for i in range(len(CHUNKS)):
        for step in range(3):
            reduce_copy(i, step).wait_send()
            gather_copy(i, step).wait_send()


def local(x_field, observed, sat_scale, u_coef, v_coef, ranks):
    tile_rows, tile_cols, width, cap = u_coef.shape
    sources = x_field.shape[1]
    hbm = pl.BlockSpec(memory_space=pltpu.HBM)
    chunks = len(CHUNKS)
    peers = len(OFFSETS)
    dma = pltpu.SemaphoreType.DMA
    half_rows = tile_cols * width // 2
    return pl.pallas_call(
        kernel,
        out_shape=jax.ShapeDtypeStruct(x_field.shape, BF16),
        in_specs=[hbm] * 6,
        out_specs=pl.BlockSpec(memory_space=pltpu.VMEM),
        scratch_shapes=[
            pltpu.VMEM((tile_cols, width, sources), BF16),
            pltpu.VMEM(u_coef.shape, BF16),
            pltpu.VMEM(v_coef.shape, BF16),
            pltpu.VMEM(observed.shape, BF16),
            pltpu.VMEM(sat_scale.shape, F32),
            pltpu.SMEM(ranks.shape, jnp.int32),
            pltpu.VMEM((tile_cols, sources, width), BF16),
            pltpu.VMEM((16, 2, 32, sources), F32),
            pltpu.VMEM((16, 32, sources), F32),
            pltpu.VMEM((16, 32, sources), BF16),
            pltpu.VMEM((peers, 32, sources), BF16),
            pltpu.VMEM((16, 2, 32, sources), BF16),
            pltpu.VMEM((tile_rows, sources, width), BF16),
            pltpu.VMEM((tile_cols * width, sources), F32),
            pltpu.VMEM((half_rows, sources), BF16),
            pltpu.VMEM((half_rows // 2, sources), BF16),
            pltpu.VMEM((half_rows // 4, sources), BF16),
            pltpu.VMEM((half_rows, sources), BF16),
            pltpu.VMEM((half_rows // 2, sources), BF16),
            pltpu.VMEM((half_rows // 4, sources), BF16),
            dma((3, tile_rows * tile_cols)),
            dma((3,)),
            dma((3,)),
            dma((3,)),
            dma((peers,)),
            dma((peers,)),
            dma((peers,)),
            dma((peers,)),
            dma((chunks, 6)),
            dma((chunks, 6)),
        ],
        compiler_params=pltpu.CompilerParams(
            collective_id=0, has_side_effects=True, vmem_limit_bytes=60 * 2**20
        ),
        name="redatum",
    )(x_field, observed, sat_scale, u_coef, v_coef, ranks)


def solution(mesh):
    return jax.shard_map(
        local,
        mesh=mesh,
        in_specs=(
            P("col", None),
            P(("row", "col"), None),
            P(),
            P("row", "col", None, None),
            P("row", "col", None, None),
            P("row", "col"),
        ),
        out_specs=P("col", None),
        check_vma=False,
    )
```

```python
import functools

import jax
import jax.numpy as jnp
from jax import lax
from jax.experimental import pallas as pl
from jax.experimental.pallas import tpu as pltpu
from jax.sharding import PartitionSpec as P

MESH = pl.DeviceIdType.MESH
F32, BF16 = jnp.float32, jnp.bfloat16

ORDERS = ((0, 1, 2), (1, 2, 0), (2, 0, 1))
UNIT = 128


def chunk_table(rows):
    sizes = [2 * UNIT] * (rows // (2 * UNIT) - 1) + [UNIT, UNIT]
    table, first = [], 0
    for i, size in enumerate(sizes):
        table.append((first, size, ORDERS[i % 3]))
        first += size
    return table


def event_order(chunks, rate=46.65e3, latency=2.6, row_bytes=512):
    free, arrivals = [0.0] * 3, {}

    def send(i, stage, now):
        _, rows, dims = chunks[i]
        step = stage if stage < 3 else 5 - stage
        d = dims[step]
        free[d] = max(free[d], now) + (rows >> (step + 1)) * row_bytes / rate
        arrivals[stage, i] = free[d] + latency

    now, order = 0.0, []
    for i, (first, rows, _) in enumerate(chunks):
        now = max(now, 0.4 + 0.26 * ((first + rows - 1) // 512))
        send(i, 0, now)
    while arrivals:
        stage, i = min(arrivals, key=lambda e: (arrivals[e], e))
        now = max(now, arrivals.pop((stage, i))) + 0.05
        if stage < 3:
            now += (chunks[i][1] >> (stage + 1)) * 0.0009
        order.append((stage, i))
        if stage < 5:
            send(i, stage + 1, now)
    return order


OFFSETS = tuple((dx, dz) for dx in (2, 1, 3, 0) for dz in (2, 1, 3, 0) if (dx, dz) != (0, 0))


def matmul(a, b):
    return lax.dot_general(a, b, (((1,), (0,)), ((), ())), preferred_element_type=F32)


def matmul_t(a, b):
    return lax.dot_general(a, b, (((1,), (1,)), ((), ())), preferred_element_type=F32)


def kernel(
    x_hbm, obs_hbm, sat_hbm, u_hbm, v_hbm, ranks_hbm, out,
    xb, ub, vb, obs, sat, ranks, xt, ct, part, recv_core, send_a, recv_a, resid, resid_t, grad,
    send1, send2, send3, recv1, recv2, recv3,
    load_sem, small_sem, core_send, core_recv, a_send, a_recv, b_send, b_recv, r_send, r_recv,
    row_send, row_recv,
):
    r, c = lax.axis_index("row"), lax.axis_index("col")
    y, zl = r // 2, r % 2
    x, zh, k = c // 8, (c % 8) // 2, c % 2
    here = x * 4 + zh
    tile_rows, tile_cols = ub.shape[0], ub.shape[1]

    row_peer = (
        (y * 2 + 1 - zl, c),
        ((y + 1 - 2 * (y % 2)) * 2 + zl, c),
        ((3 - y) * 2 + zl, c),
    )
    bits = (zl, ((y + 1) // 2) % 2, y // 2)
    core_peer = (r, c + 1 - 2 * k)

    def chip_at(dx, dz):
        return ((x + dx) % 4) * 4 + (zh + dz) % 4

    barrier = pltpu.get_barrier_semaphore()
    peers = [core_peer, *row_peer] + [(r, chip_at(dx, dz) * 2 + k) for dx, dz in OFFSETS]
    for peer in peers:
        pl.semaphore_signal(barrier, inc=1, device_id=peer, device_id_type=MESH)

    def load(n, a, p):
        tiles = pl.ds(p * 2, 2)
        if n == 2:
            return pltpu.make_async_copy(
                x_hbm.at[pl.ds(p * 1024, 1024)], xb.at[pl.ds(p * 1024, 1024)], load_sem.at[2, 0, p]
            )
        source, target = ((v_hbm, vb), (u_hbm, ub))[n]
        return pltpu.make_async_copy(source.at[a, tiles], target.at[a, tiles], load_sem.at[n, a, p])

    pieces = tile_cols // 2
    xs = [load(2, 0, p) for p in range(pieces)]
    vs = [load(0, a, p) for a in range(tile_rows) for p in range(pieces)]
    us = [load(1, a, p) for a in range(tile_rows) for p in range(pieces)]
    small = (
        pltpu.make_async_copy(ranks_hbm, ranks, small_sem.at[0]),
        pltpu.make_async_copy(obs_hbm, obs, small_sem.at[1]),
        pltpu.make_async_copy(sat_hbm, sat, small_sem.at[2]),
    )
    small[0].start()
    for copy in xs + vs + us:
        copy.start()
    small[1].start()
    small[2].start()

    eye = (
        lax.broadcasted_iota(jnp.int32, (256, 256), 0) == lax.broadcasted_iota(jnp.int32, (256, 256), 1)
    ).astype(F32).astype(BF16)
    lane = lax.broadcasted_iota(jnp.int32, (256, 256), 1)

    def masked(value, a, j):
        return jnp.where(lane < ranks[a, j], value, 0.0).astype(BF16)

    for copy in (small[0], *xs, *vs):
        copy.wait()
    for j in range(tile_cols):
        xt[j] = matmul_t(eye, xb[pl.ds(j * 512, 512)]).astype(BF16)
    for j in range(tile_cols):
        for a in range(tile_rows):
            ct[a, j] = masked(matmul(xt[j], vb[a, j]), a, j)
    for copy in us:
        copy.wait()
    core_copies = []
    for a in range(tile_rows):
        blocks = pl.ds(a * 8, 8)
        for j in range(0, tile_cols, 2):
            term = (matmul_t(ub[a, j], ct[a, j]) + matmul_t(ub[a, j + 1], ct[a, j + 1])).reshape(8, 2, 32, 256)
            if j == 0:
                part[blocks] = term
            else:
                part[blocks] += term
        if a == 0:
            pl.semaphore_wait(barrier, len(peers))
        copy = pltpu.make_async_remote_copy(
            src_ref=part.at[pl.ds(a * 8, 8), 1 - k],
            dst_ref=recv_core.at[pl.ds(a * 8, 8)],
            send_sem=core_send.at[a],
            recv_sem=core_recv.at[a],
            device_id=core_peer,
            device_id_type=MESH,
        )
        copy.start()
        core_copies.append(copy)

    a_copies = []
    for a in range(tile_rows):
        core_copies[a].wait_recv()
        blocks = pl.ds(a * 8, 8)
        send_a[blocks] = (part[blocks, k] + recv_core[blocks]).astype(BF16)
    for n, (dx, dz) in enumerate(OFFSETS):
        there = chip_at(dx, dz)
        copy = pltpu.make_async_remote_copy(
            src_ref=send_a.at[there],
            dst_ref=recv_a.at[n],
            send_sem=a_send.at[n],
            recv_sem=a_recv.at[n],
            device_id=(r, there * 2 + k),
            device_id_type=MESH,
        )
        copy.start()
        a_copies.append(copy)

    small[1].wait()
    small[2].wait()
    predicted = part[here, k] + recv_core[here]
    for n, copy in enumerate(a_copies):
        copy.wait_recv()
        predicted = predicted + recv_a[n].astype(F32)
    scale = sat[...].reshape(1, 256)
    misfit = (predicted - obs[...].astype(F32)) / scale
    resid[here, k] = (scale * jnp.tanh(misfit)).astype(BF16)

    b_copies = []
    for n, (dx, dz) in enumerate(OFFSETS):
        copy = pltpu.make_async_remote_copy(
            src_ref=resid.at[here, k],
            dst_ref=resid.at[here, k],
            send_sem=b_send.at[n],
            recv_sem=b_recv.at[n],
            device_id=(r, chip_at(dx, dz) * 2 + k),
            device_id_type=MESH,
        )
        copy.start()
        b_copies.append(copy)
    for copy in core_copies + a_copies:
        copy.wait_send()
    r_copies = []
    for dx in (0, 1, 3, 2):
        for n, offset in enumerate(OFFSETS):
            if offset[0] == (4 - dx) % 4:
                b_copies[n].wait_recv()
        blocks = pl.ds(((x + dx) % 4) * 4, 4)
        copy = pltpu.make_async_remote_copy(
            src_ref=resid.at[blocks, k],
            dst_ref=resid.at[blocks, k],
            send_sem=r_send.at[dx],
            recv_sem=r_recv.at[dx],
            device_id=core_peer,
            device_id_type=MESH,
        )
        copy.start()
        r_copies.append(copy)
    for other in b_copies:
        other.wait_send()
    for copy in r_copies:
        copy.wait()

    for a in range(tile_rows):
        resid_t[a] = matmul_t(eye, resid[pl.ds(a * 8, 8)].reshape(512, 256)).astype(BF16)

    chunks = chunk_table(grad.shape[0])
    sends = [(send1, recv1), (send2, recv2), (send3, recv3)]

    def base_of(i, depth):
        first, rows, dims = chunks[i]
        base = first
        for d in range(depth):
            base = base + bits[dims[d]] * (rows >> (d + 1))
        return base if depth == 0 else pl.multiple_of(base, 16)

    def reduce_copy(i, step):
        first, rows, dims = chunks[i]
        slot = pl.ds(first >> (step + 1), rows >> (step + 1))
        return pltpu.make_async_remote_copy(
            src_ref=sends[step][0].at[slot],
            dst_ref=sends[step][1].at[slot],
            send_sem=row_send.at[i, step],
            recv_sem=row_recv.at[i, step],
            device_id=row_peer[dims[step]],
            device_id_type=MESH,
        )

    def gather_copy(i, step):
        first, rows, dims = chunks[i]
        where = pl.ds(base_of(i, step + 1), rows >> (step + 1))
        return pltpu.make_async_remote_copy(
            src_ref=out.at[where],
            dst_ref=out.at[where],
            send_sem=row_send.at[i, 3 + step],
            recv_sem=row_recv.at[i, 3 + step],
            device_id=row_peer[dims[step]],
            device_id_type=MESH,
        )

    def send_part(i, step):
        first, rows, dims = chunks[i]
        half = rows >> (step + 1)
        bit = bits[dims[step]]
        theirs = pl.multiple_of((1 - bit) * half, 16)
        base = base_of(i, step)
        value = grad[pl.ds(pl.multiple_of(base + theirs, 16), half)]
        slot = first >> (step + 1)
        if step > 0:
            value = value + sends[step - 1][1][pl.ds(pl.multiple_of((first >> step) + theirs, 16), half)].astype(F32)
        sends[step][0][pl.ds(slot, half)] = value.astype(BF16)
        reduce_copy(i, step).start()
        if step > 0:
            mine = pl.multiple_of(bit * half, 16)
            keep = pl.ds(pl.multiple_of(base + mine, 16), half)
            grad[keep] = grad[keep] + sends[step - 1][1][
                pl.ds(pl.multiple_of((first >> step) + mine, 16), half)
            ].astype(F32)

    sent = 0
    for j in range(tile_cols):
        total = None
        for a in range(tile_rows):
            adjoint = masked(matmul(resid_t[a], ub[a, j]), a, j)
            term = matmul_t(vb[a, j], adjoint)
            total = term if total is None else total + term
        grad[pl.ds(j * 512, 512)] = total
        while sent < len(chunks) and chunks[sent][0] + chunks[sent][1] <= (j + 1) * 512:
            send_part(sent, 0)
            sent += 1

    for stage, i in event_order(chunks):
        first, rows, dims = chunks[i]
        if stage < 2:
            reduce_copy(i, stage).wait_recv()
            send_part(i, stage + 1)
        elif stage == 2:
            reduce_copy(i, 2).wait_recv()
            where = pl.ds(base_of(i, 3), rows >> 3)
            out[where] = (grad[where] + recv3[pl.ds(first >> 3, rows >> 3)].astype(F32)).astype(BF16)
            gather_copy(i, 2).start()
        else:
            step = 5 - stage
            gather_copy(i, step).wait_recv()
            if step > 0:
                gather_copy(i, step - 1).start()
    for i in range(len(chunks)):
        for step in range(3):
            reduce_copy(i, step).wait_send()
            gather_copy(i, step).wait_send()


def local(x_field, observed, sat_scale, u_coef, v_coef, ranks):
    arrays = (x_field, observed, sat_scale, u_coef, v_coef, ranks)
    tile_rows, tile_cols, width, cap = u_coef.shape
    sources = x_field.shape[1]
    hbm = pl.BlockSpec(memory_space=pltpu.HBM)
    chunks = len(chunk_table(x_field.shape[0]))
    peers = len(OFFSETS)
    dma = pltpu.SemaphoreType.DMA
    half_rows = tile_cols * width // 2
    return pl.pallas_call(
        kernel,
        out_shape=jax.ShapeDtypeStruct(x_field.shape, BF16),
        in_specs=[hbm] * 6,
        out_specs=pl.BlockSpec(memory_space=pltpu.VMEM),
        scratch_shapes=[
            pltpu.VMEM(x_field.shape, BF16),
            pltpu.VMEM(u_coef.shape, BF16),
            pltpu.VMEM(v_coef.shape, BF16),
            pltpu.VMEM(observed.shape, BF16),
            pltpu.VMEM(sat_scale.shape, F32),
            pltpu.SMEM(ranks.shape, jnp.int32),
            pltpu.VMEM((tile_cols, sources, width), BF16),
            pltpu.VMEM((tile_rows, tile_cols, sources, cap), BF16),
            pltpu.VMEM((16, 2, 32, sources), F32),
            pltpu.VMEM((16, 32, sources), F32),
            pltpu.VMEM((16, 32, sources), BF16),
            pltpu.VMEM((peers, 32, sources), BF16),
            pltpu.VMEM((16, 2, 32, sources), BF16),
            pltpu.VMEM((tile_rows, sources, width), BF16),
            pltpu.VMEM((tile_cols * width, sources), F32),
            pltpu.VMEM((half_rows, sources), BF16),
            pltpu.VMEM((half_rows // 2, sources), BF16),
            pltpu.VMEM((half_rows // 4, sources), BF16),
            pltpu.VMEM((half_rows, sources), BF16),
            pltpu.VMEM((half_rows // 2, sources), BF16),
            pltpu.VMEM((half_rows // 4, sources), BF16),
            dma((3, tile_rows, tile_cols // 2)),
            dma((3,)),
            dma((tile_rows,)),
            dma((tile_rows,)),
            dma((peers,)),
            dma((peers,)),
            dma((peers,)),
            dma((peers,)),
            dma((4,)),
            dma((4,)),
            dma((chunks, 6)),
            dma((chunks, 6)),
        ],
        compiler_params=pltpu.CompilerParams(
            collective_id=0, has_side_effects=True, vmem_limit_bytes=36 * 2**20
        ),
        name="redatum",
    )(*(pltpu.with_memory_space_constraint(array, pltpu.HBM) for array in arrays))


def solution(mesh):
    return jax.shard_map(
        local,
        mesh=mesh,
        in_specs=(
            P("col", None),
            P(("row", "col"), None),
            P(),
            P("row", "col", None, None),
            P("row", "col", None, None),
            P("row", "col"),
        ),
        out_specs=P("col", None),
        check_vma=False,
    )
```
